512 devices in a mesh: rep: 4 (over y), ep: 128 (over z, x, core).
Axes of the slice: x: 4, y: 4, z: 16, core: 2. Of those that a mesh axis runs over, the one named last changes fastest.
Arguments:
- gen_cache: bfloat16 [4096, 32, 2, 4, 128], P(('rep', 'ep')), may hold values from -6 to 6
- prompt_cache: bfloat16 [256, 2, 4, 128], replicated, may hold values from -5 to 5
- ancestors: int32 [4096], P(('rep', 'ep')), may hold values from 0 to 1023, as said below
- queries: bfloat16 [4096, 2, 64, 128], P(('rep', 'ep')), may hold values from -5 to 5
- new_kv: bfloat16 [4096, 2, 2, 4, 128], P(('rep', 'ep')), may hold values from -6 to 6
- tokens_in: bfloat16 [4096, 2, 2048], P(('rep', 'ep')), may hold values from -6 to 6
- norm_gain: float32 [2048], replicated, may hold values from 0.1 to 1.9
- routes: int32 [4, 1024, 2, 8], P(None, 'ep'), may hold values from 0 to 127, all different within a row; in each aligned block of 16 rows (0 to 15, 16 to 31, ..., all dimensions but the last counted through in order) at most 2 rows name the same one
- gate_weights: float32 [4, 1024, 2, 8], P(None, 'ep'), may hold values from 0.1 to 1
- w_gate_up: bfloat16 [128, 2048, 2, 768], P('ep', None, None, 'rep'), may hold values from -0.125 to 0.125
- w_down: bfloat16 [128, 768, 2048], P('ep', 'rep'), may hold values from -0.21875 to 0.21875
Outputs:
- cache_out: bfloat16 [4096, 32, 2, 4, 128], P(('rep', 'ep'))
- attn_out: bfloat16 [4096, 2, 64, 128], P(('rep', 'ep'))
- expert_out: bfloat16 [4096, 2, 2048], P(('rep', 'ep'))
The draws below stay inside these ranges and needn't reach their ends.
Inputs may be any that keep to these rules, and one draw needn't show every extreme that they name: The parent of particle p is particle (p // 1024) * 1024 + ancestors[p]. `routes`: each row names 8 different experts. In the rows of one device (aligned blocks of 16 rows, taking the leading dimensions together in order) no expert is named more than 2 times.
All inputs are finite; a program needn't handle non-finite values.
Results may differ from the reference program's by a relative error of at most 0.013.
Values may be sent and summed in bfloat16 or wider, within the bound.
No kernel may reach another device: no remote copies, remote signals or barrier semaphores. Data moves between devices by JAX's collectives and lax.ppermute only.
A program may use at most 64 MiB of HBM per device.

```python
import functools
import math
import jax
import jax.numpy as jnp
import numpy as np
from jax import lax

D = 2048
HID = 768
QH = 64
KVH = 4
HD = 128
TOP = 8
P_SIZE = 256
G = 32
PD = 8
GROUP = 1024
PARTICLES = 4096
EXPERTS = 128
HSLICE = 192
MOST = 2
N_REP = 4
DEVICES = 512


def query_parts(key):
    base = jnp.clip(jax.random.normal(jax.random.fold_in(key, 101), (PARTICLES, 2, QH, HD), jnp.float32), -5.0, 5.0)
    final = base
    return (base, final)


def draw_queries(key, part):
    return query_parts(key)[1].astype(jnp.bfloat16)


def draw_new_kv(key, part):
    base = query_parts(key)[0]
    grouped = jnp.mean(base.reshape(PARTICLES, 2, KVH, QH // KVH, HD), axis=3)
    noise = jax.random.normal(jax.random.fold_in(key, 111), (PARTICLES, 2, KVH, HD), jnp.float32)
    new_keys = jnp.clip(4.0 * grouped + 0.5 * noise, -6.0, 6.0)
    new_values = jnp.clip(jax.random.normal(jax.random.fold_in(key, 112), (PARTICLES, 2, KVH, HD), jnp.float32), -6.0, 6.0)
    return jnp.stack([new_keys, new_values], axis=2).astype(jnp.bfloat16)


def draw_prompt_cache(key, part):
    values = jnp.clip(jax.random.normal(jax.random.fold_in(key, 121), (P_SIZE, 2, KVH, HD), jnp.float32), -5.0, 5.0)
    return values.astype(jnp.bfloat16)


def draw_ancestors(key, part):
    groups = PARTICLES // GROUP
    first = jax.random.randint(jax.random.fold_in(key, 201), (PARTICLES,), 0, GROUP, dtype=jnp.int32)
    second = jax.random.randint(jax.random.fold_in(key, 202), (PARTICLES,), 0, GROUP, dtype=jnp.int32)
    skewed = first * second // GROUP
    even = jax.random.randint(jax.random.fold_in(key, 203), (PARTICLES,), 0, GROUP, dtype=jnp.int32)
    coins = jax.random.randint(jax.random.fold_in(key, 204), (PARTICLES,), 0, 2, dtype=jnp.int32)
    picked = jnp.where(coins == 1, skewed, even)
    labels = jax.vmap(lambda subkey: jax.random.permutation(subkey, GROUP))(jax.random.split(jax.random.fold_in(key, 205), groups)).astype(jnp.int32)
    group_of = jnp.arange(PARTICLES, dtype=jnp.int32) // GROUP
    local = jnp.arange(PARTICLES, dtype=jnp.int32) % GROUP
    result = labels[group_of, picked]
    spot_high = jax.random.randint(jax.random.fold_in(key, 206), (groups,), 0, GROUP, dtype=jnp.int32)
    offset = jax.random.randint(jax.random.fold_in(key, 207), (groups,), 1, GROUP, dtype=jnp.int32)
    spot_low = (spot_high + offset) % GROUP
    result = jnp.where(local == spot_high[group_of], GROUP - 1, result)
    result = jnp.where(local == spot_low[group_of], 0, result)
    return result.astype(jnp.int32)


def levels(own_key, dims, cuts, smallest, largest):
    loudness, own = 1.0, jax.random.fold_in(own_key, 6)
    for axis_at, blocks in cuts:
        heights = jnp.exp(jax.random.uniform(jax.random.fold_in(own, axis_at), (blocks,), jnp.float32, smallest / len(cuts), largest / len(cuts)))
        loudness = loudness * jnp.repeat(heights, dims[axis_at] // blocks).reshape([-1 if axis == axis_at else 1 for axis in range(len(dims))])
    return loudness


def shared_out(rng, own, number, rows, number_of, top, reach, slope):
    ranking = jax.random.permutation(rng, number_of)
    packed, ordinary = shares(number_of, rows * top, reach, slope, True), shares(number_of, rows * top, reach, slope, False)
    places = jnp.arange(number_of)

    def named(sizes, turn):
        used = int((sizes > 0).sum())
        fixed = max(1, used // 4)
        shifted = fixed + (places - fixed + turn * (used - fixed)) % max(1, number_of - fixed)
        return jnp.zeros((number_of,), jnp.int32).at[ranking[jnp.where(places < fixed, places, shifted)]].set(jnp.asarray(sizes, jnp.int32))

    sizes = jnp.where(number % 4 == 0, named(packed, number // 4), named(ordinary, number - number // 4 - 1))
    mixed = jax.random.permutation(jax.random.fold_in(own, 3), number_of)
    source_of, receiver = mixed[0:number_of // 2 * 2:2], mixed[1:number_of // 2 * 2:2]
    slack = jnp.minimum(sizes[source_of] - 1, reach - sizes[receiver]) // 2
    slack = jnp.where((source_of == ranking[0]) | (receiver == ranking[0]) | (sizes[receiver] == 0), 0, jnp.maximum(slack, 0))
    shifted = jax.random.randint(jax.random.fold_in(own, 4), (number_of // 2,), 0, 1 << 20) % (slack + 1)
    sizes = sizes.at[source_of].add(-shifted).at[receiver].add(shifted)
    items = jnp.searchsorted(jnp.cumsum(sizes), jnp.arange(rows * top), side="right").astype(jnp.int32)
    table = items.reshape(top, rows).T
    table = table[jax.random.permutation(jax.random.fold_in(own, 1), rows)]
    turn = jax.random.randint(jax.random.fold_in(own, 2), (rows, 1), 0, top)
    return jnp.take_along_axis(table, (jnp.arange(top)[None, :] + turn) % top, axis=1)


def shares(count, total, most, skew, full):
    weights = [(1 << 20) // math.isqrt(standing ** skew) + 1 for standing in range(1, count + 1)]
    largest = most if full else min(most, max(-(-total // count), total * weights[0] // sum(weights)))
    least = 1 if total - largest >= count - 1 else 0
    given, spare = [largest] + [least] * (count - 1), total - largest - least * (count - 1)
    while spare > 0:
        movable = [i for i in range(1, count) if given[i] < largest] or [i for i in range(1, count) if given[i] < most]
        pool, left = sum([weights[i] for i in movable]), spare
        for i in movable:
            addition = min(most - given[i], max(1, left * weights[i] // pool), spare)
            given[i] = given[i] + addition
            spare = spare - addition
    return np.array(given)


def scatter_about(key, dims, spread, reach, cuts=(), held_as=jnp.bfloat16):
    gain = levels(key, dims, cuts, -0.22, 0.18) if cuts else 1.0
    entries = jax.random.normal(key, dims, jnp.float32) * spread * gain
    return jnp.minimum(jnp.maximum(entries, -reach), reach).astype(held_as)


def setup_inputs(seed: int = 0) -> dict:
    keys = jax.random.split(jax.random.key(seed), 12)
    gen_cache = scatter_about(keys[0], (PARTICLES, G, 2, KVH, HD), 1.0, 6.0, ((0, 512),))
    prompt_cache = draw_prompt_cache(jax.random.fold_in(keys[11], 71), 0)
    ancestors = draw_ancestors(jax.random.fold_in(keys[11], 71), 0)
    queries = draw_queries(jax.random.fold_in(keys[11], 71), 0)
    new_kv = draw_new_kv(jax.random.fold_in(keys[11], 71), 0)
    tokens_in = scatter_about(keys[5], (PARTICLES, 2, D), 1.0, 6.0, ((0, 512),))
    norm_gain = jnp.clip(1.0 + 0.18 * jax.random.normal(keys[6], (D,), jnp.float32), 0.1, 1.9)
    routes_keys = jax.random.split(jax.random.fold_in(keys[7], 1), N_REP * GROUP * 2 // (2 * PD))
    routes_turns = jax.random.permutation(jax.random.fold_in(keys[7], 3), N_REP * GROUP * 2 // (2 * PD))
    routes = jax.vmap(lambda own, number: shared_out(jax.random.fold_in(keys[7], 2), own, number, 2 * PD, EXPERTS, TOP, MOST, 2))(routes_keys, routes_turns).reshape((N_REP, GROUP, 2, TOP))
    gate_weights = jnp.clip(jnp.exp(math.log(1.0) - 2.3025851 * jax.random.uniform(keys[8], (N_REP, GROUP, 2, TOP), jnp.float32) ** levels(keys[8], (N_REP, GROUP, 2, TOP), ((1, 128),), -0.2, 0.2)), 0.1, 1.0)
    w_gate_up = scatter_about(keys[9], (EXPERTS, D, 2, HID), D ** -0.5, 0.125, ((0, 128), (3, 4)))
    w_down = scatter_about(keys[10], (EXPERTS, HID, D), HID ** -0.5, 0.21875, ((0, 128), (1, 4)))
    return {"gen_cache": gen_cache, "prompt_cache": prompt_cache, "ancestors": ancestors, "queries": queries, "new_kv": new_kv, "tokens_in": tokens_in, "norm_gain": norm_gain, "routes": routes, "gate_weights": gate_weights, "w_gate_up": w_gate_up, "w_down": w_down}


def attend_block(inputs, prompt_cache):
    queries, gen_block, new_block = inputs
    count = queries.shape[0]
    group_heads = QH // KVH
    score_scale = 1.0 / math.sqrt(HD)
    query_f = queries.astype(jnp.float32).reshape(count, 2, KVH, group_heads, HD)
    prompt_keys = prompt_cache[:, 0].astype(jnp.float32)
    prompt_values = prompt_cache[:, 1].astype(jnp.float32)
    gen_keys = gen_block[:, :, 0].astype(jnp.float32)
    gen_values = gen_block[:, :, 1].astype(jnp.float32)
    new_keys = new_block[:, :, 0].astype(jnp.float32)
    new_values = new_block[:, :, 1].astype(jnp.float32)
    prompt_scores = jnp.einsum('btngd,snd->btngs', query_f, prompt_keys) * score_scale
    gen_scores = jnp.einsum('btngd,bsnd->btngs', query_f, gen_keys) * score_scale
    new_scores = jnp.einsum('btngd,bsnd->btngs', query_f, new_keys) * score_scale
    causal = lax.broadcasted_iota(jnp.int32, (2, 2), 1) <= lax.broadcasted_iota(jnp.int32, (2, 2), 0)
    new_scores = jnp.where(causal[None, :, None, None, :], new_scores, -jnp.inf)
    row_max = jnp.maximum(jnp.maximum(prompt_scores.max(-1), gen_scores.max(-1)), new_scores.max(-1))[..., None]
    prompt_exp = jnp.exp(prompt_scores - row_max)
    gen_exp = jnp.exp(gen_scores - row_max)
    new_exp = jnp.exp(new_scores - row_max)
    denom = (prompt_exp.sum(-1) + gen_exp.sum(-1) + new_exp.sum(-1))[..., None]
    prompt_weights = lax.optimization_barrier((prompt_exp / denom).astype(jnp.bfloat16)).astype(jnp.float32)
    gen_weights = lax.optimization_barrier((gen_exp / denom).astype(jnp.bfloat16)).astype(jnp.float32)
    new_weights = lax.optimization_barrier((new_exp / denom).astype(jnp.bfloat16)).astype(jnp.float32)
    result = jnp.einsum('btngs,snd->btngd', prompt_weights, prompt_values)
    result = result + jnp.einsum('btngs,bsnd->btngd', gen_weights, gen_values)
    result = result + jnp.einsum('btngs,bsnd->btngd', new_weights, new_values)
    return result.reshape(count, 2, QH, HD).astype(jnp.bfloat16)

def reference(gen_cache, prompt_cache, ancestors, queries, new_kv, tokens_in, norm_gain, routes, gate_weights, w_gate_up, w_down):
    particle_ids = jnp.arange(PARTICLES, dtype=jnp.int32)
    parent = (particle_ids // GROUP * GROUP + ancestors).astype(jnp.int32)
    cache_out = jnp.take(gen_cache, parent, axis=0)
    blocks = PARTICLES // PD
    inputs = (queries.reshape(blocks, PD, 2, QH, HD), cache_out.reshape(blocks, PD, G, 2, KVH, HD), new_kv.reshape(blocks, PD, 2, 2, KVH, HD))
    attn_out = lax.map(functools.partial(attend_block, prompt_cache=prompt_cache), inputs).reshape(PARTICLES, 2, QH, HD)
    row_count = PARTICLES * 2
    values_f = tokens_in.astype(jnp.float32).reshape(row_count, D)
    normed = (values_f * lax.rsqrt(lax.optimization_barrier(jnp.mean(values_f * values_f, axis=-1, keepdims=True)) + 1e-06) * norm_gain).astype(jnp.bfloat16)
    route_flat = routes.reshape(row_count * TOP).astype(jnp.int32)
    weight_flat = gate_weights.reshape(row_count * TOP)
    capacity = min(row_count, DEVICES * MOST)

    def one_expert(summed, expert):
        chosen = route_flat == expert
        found = jnp.sum(chosen.astype(jnp.int32))
        positions = jnp.nonzero(chosen, size=capacity, fill_value=0)[0].astype(jnp.int32)
        valid = jnp.arange(capacity, dtype=jnp.int32) < found
        rows = (positions // TOP).astype(jnp.int32)
        gates = jnp.where(valid, jnp.take(weight_flat, positions), 0.0)
        inputs_e = jnp.take(normed, rows, axis=0)
        weights_e = lax.dynamic_index_in_dim(w_gate_up, expert, 0, keepdims=False)
        gate = jnp.dot(inputs_e, weights_e[:, 0, :], preferred_element_type=jnp.float32)
        upward = jnp.dot(inputs_e, weights_e[:, 1, :], preferred_element_type=jnp.float32)
        act = (jax.nn.silu(gate) * upward).astype(jnp.bfloat16)
        down_e = lax.dynamic_index_in_dim(w_down, expert, 0, keepdims=False)
        parts = jnp.einsum('crh,rhd->crd', act.astype(jnp.float32).reshape(capacity, N_REP, HSLICE), down_e.astype(jnp.float32).reshape(N_REP, HSLICE, D))
        parts = parts.astype(jnp.bfloat16).astype(jnp.float32)
        full = lax.optimization_barrier(jnp.sum(parts, axis=1)) * gates[:, None]
        return (summed.at[rows].add(full), None)
    start = jnp.zeros((row_count, D), jnp.float32)
    summed, _ = lax.scan(one_expert, start, jnp.arange(EXPERTS, dtype=jnp.int32))
    expert_out = summed.astype(jnp.bfloat16).reshape(PARTICLES, 2, D)
    return (cache_out, attn_out, expert_out)
```

```python
import math

import jax
import jax.numpy as jnp
from jax import lax
from jax.experimental import pallas as pl
from jax.experimental.pallas import tpu as pltpu
from jax.sharding import Mesh
from jax.sharding import PartitionSpec as P


EP = ("ep_0", "ep_1", "ep_2")
REP_EP = ("rep", "ep_0", "ep_1", "ep_2")


def shift(block, axis, count, step):
    return lax.ppermute(block, axis, [(i, (i + step) % count) for i in range(count)])


def ring_gather(block):
    half = block.shape[0] // 2
    before = shift(block, "rep", 4, 1)
    after = shift(block, "rep", 4, -1)
    far_low = shift(before[:half], "rep", 4, 1)
    far_high = shift(after[half:], "rep", 4, -1)
    return before, after, far_low, far_high


def ring_rows(block):
    wide = [block] + [shift(block, "ep_0", 16, step) for step in (4, -4, 8)]
    wide = jnp.concatenate(wide, axis=0)
    return [wide] + [shift(wide, "ep_0", 16, step) for step in (1, -1, 2)]


def select_body(place_ref, own_ref, back_ref, ahead_ref, far_ref, out_ref, rows_ref, *, width):
    for n, part in enumerate((own_ref, back_ref, ahead_ref, far_ref)):
        rows_ref[n * 64 : (n + 1) * 64, :] = part[...]
    count = rows_ref.shape[0]
    slots = out_ref.shape[0]
    place = place_ref[0]
    row = lax.broadcasted_iota(jnp.int32, (count, 1), 0)
    near, wide = row // 64, row // 16 % 4
    distance = jnp.where(near == 1, -1, jnp.where(near == 2, 1, jnp.where(near == 3, -2, 0)))
    distance += jnp.where(wide == 1, -4, jnp.where(wide == 2, 4, jnp.where(wide == 3, -8, 0)))
    source = (place + distance + 16) % 16
    column = lax.broadcasted_iota(jnp.int32, (count, slots), 1)
    expert = place * 8 + column // 32
    ids = rows_ref[:, width:].astype(jnp.int32)
    named = ids[:, 0:1] == expert
    for k in range(1, 8):
        named = named | (ids[:, k : k + 1] == expert)
    lower = lax.broadcasted_iota(jnp.int32, (count, count), 0)
    upper = lax.broadcasted_iota(jnp.int32, (count, count), 1)
    earlier = (upper < lower) & (upper // 16 == lower // 16)
    rank = jnp.dot(
        earlier.astype(jnp.float32).astype(jnp.bfloat16),
        named.astype(jnp.float32).astype(jnp.bfloat16),
        preferred_element_type=jnp.float32,
    ).astype(jnp.int32)
    chosen = named & (source * 2 + rank == column % 32)
    out_ref[...] = lax.dot_general(
        chosen.astype(jnp.float32).astype(jnp.bfloat16),
        rows_ref[:, :width],
        (((0,), (0,)), ((), ())),
        preferred_element_type=jnp.float32,
    ).astype(jnp.bfloat16)


def select_rows(place, blocks, width, slots):
    rows = sum(b.shape[0] for b in blocks)
    spec = pl.BlockSpec(memory_space=pltpu.VMEM)
    return pl.pallas_call(
        lambda *refs: select_body(*refs, width=width),
        out_shape=jax.ShapeDtypeStruct((slots, width), jnp.bfloat16),
        in_specs=[pl.BlockSpec(memory_space=pltpu.SMEM)] + [spec] * 4,
        out_specs=spec,
        scratch_shapes=[pltpu.VMEM((rows, blocks[0].shape[1]), jnp.bfloat16)],
        name="select_rows",
    )(place.reshape(1), *blocks)


def expert_body(
    rows_hbm, in_hbm, out_hbm, before_hbm, after_hbm, low_hbm, high_hbm, result_hbm,
    rows, own, before, after, far, result, sems,
):
    hidden = own.shape[0] // 3
    half = low_hbm.shape[0]
    copies = [
        pltpu.make_async_copy(src, dst, sems.at[n])
        for n, (src, dst) in enumerate(
            (
                (rows_hbm, rows),
                (in_hbm, own.at[: 2 * hidden]),
                (out_hbm, own.at[2 * hidden :]),
                (before_hbm, before),
                (after_hbm, after),
                (low_hbm, far.at[:half]),
                (high_hbm, far.at[half:]),
            )
        )
    ]
    for copy in copies:
        copy.start()
    count = rows.shape[0]
    to = lax.broadcasted_iota(jnp.int32, (count, count), 0)
    come = lax.broadcasted_iota(jnp.int32, (count, count), 1)
    order = come == to // 2 % 8 * 32 + to // 16 * 2 + to % 2
    order = order.astype(jnp.float32).astype(jnp.bfloat16)
    total = None
    contract = (((1,), (1,)), ((), ()))
    for weights, waits in ((own, (0, 1, 2)), (before, (3,)), (after, (4,)), (far, (5, 6))):
        for n in waits:
            copies[n].wait()
        both = lax.dot_general(
            rows[...], weights[: 2 * hidden], contract, preferred_element_type=jnp.float32
        )
        gate, upward = both[:, :hidden], both[:, hidden:]
        act = (gate / (1.0 + jnp.exp(-gate)) * upward).astype(jnp.bfloat16)
        act = jnp.dot(order, act, preferred_element_type=jnp.float32).astype(jnp.bfloat16)
        part = jnp.dot(act, weights[2 * hidden :], preferred_element_type=jnp.float32)
        total = part if total is None else total + part
    result[...] = total.astype(jnp.bfloat16)
    last = pltpu.make_async_copy(result, result_hbm, sems.at[7])
    last.start()
    last.wait()


def expert(rows, in_own, out_own, before, after, low, high):
    count, width = rows.shape
    span = before.shape[0]
    return pl.pallas_call(
        expert_body,
        out_shape=jax.ShapeDtypeStruct((count, width), jnp.bfloat16),
        in_specs=[pl.BlockSpec(memory_space=pl.ANY)] * 7,
        out_specs=pl.BlockSpec(memory_space=pl.ANY),
        scratch_shapes=[pltpu.VMEM((count, width), jnp.bfloat16)]
        + [pltpu.VMEM((span, width), jnp.bfloat16)] * 4
        + [pltpu.VMEM((count, width), jnp.bfloat16), pltpu.SemaphoreType.DMA((8,))],
        compiler_params=pltpu.CompilerParams(vmem_limit_bytes=32 * 1024 * 1024),
        name="expert",
    )(rows, in_own, out_own, before, after, low, high)


def attend(queries, gen_block, new_block, prompt_cache):
    count = queries.shape[0]
    heads = queries.shape[2]
    head_dim = queries.shape[3]
    kv_heads = new_block.shape[3]
    score_scale = 1.0 / math.sqrt(head_dim)
    grouped = queries.reshape(count, 2, kv_heads, heads // kv_heads, head_dim)
    prompt_scores = (
        jnp.einsum(
            "btngd,snd->btngs", grouped, prompt_cache[:, 0], preferred_element_type=jnp.float32
        )
        * score_scale
    )
    gen_scores = (
        jnp.einsum(
            "btngd,bsnd->btngs", grouped, gen_block[:, :, 0], preferred_element_type=jnp.float32
        )
        * score_scale
    )
    new_scores = (
        jnp.einsum(
            "btngd,bsnd->btngs", grouped, new_block[:, :, 0], preferred_element_type=jnp.float32
        )
        * score_scale
    )
    causal = lax.broadcasted_iota(jnp.int32, (2, 2), 1) <= lax.broadcasted_iota(
        jnp.int32, (2, 2), 0
    )
    new_scores = jnp.where(causal[None, :, None, None, :], new_scores, -jnp.inf)
    row_max = jnp.maximum(
        jnp.maximum(prompt_scores.max(-1), gen_scores.max(-1)), new_scores.max(-1)
    )[..., None]
    prompt_exp = jnp.exp(prompt_scores - row_max)
    gen_exp = jnp.exp(gen_scores - row_max)
    new_exp = jnp.exp(new_scores - row_max)
    denom = (prompt_exp.sum(-1) + gen_exp.sum(-1) + new_exp.sum(-1))[..., None]
    prompt_weights = (prompt_exp / denom).astype(jnp.bfloat16)
    gen_weights = (gen_exp / denom).astype(jnp.bfloat16)
    new_weights = (new_exp / denom).astype(jnp.bfloat16)
    result = jnp.einsum(
        "btngs,snd->btngd", prompt_weights, prompt_cache[:, 1], preferred_element_type=jnp.float32
    )
    result = result + jnp.einsum(
        "btngs,bsnd->btngd", gen_weights, gen_block[:, :, 1], preferred_element_type=jnp.float32
    )
    result = result + jnp.einsum(
        "btngs,bsnd->btngd", new_weights, new_block[:, :, 1], preferred_element_type=jnp.float32
    )
    return result.reshape(count, 2, heads, head_dim).astype(jnp.bfloat16)


def slot_numbers(expert_ids, capacity):
    flat_ids = expert_ids.reshape(-1)
    count = flat_ids.shape[0]
    earlier = lax.broadcasted_iota(jnp.int32, (count, count), 1) < lax.broadcasted_iota(
        jnp.int32, (count, count), 0
    )
    same = (flat_ids[:, None] == flat_ids[None, :]) & earlier
    rank = jnp.sum(same.astype(jnp.int32), axis=1)
    return (flat_ids * capacity + rank).reshape(expert_ids.shape)


def shards(
    gen_cache,
    prompt_cache,
    ancestors,
    queries,
    new_kv,
    tokens_in,
    norm_gain,
    routes,
    gate_weights,
    w_gate_up,
    w_down,
):
    ep_count = lax.axis_size(EP)
    per_dev = gen_cache.shape[0]
    row_count = 2 * per_dev
    width = tokens_in.shape[2]
    top_count = routes.shape[3]
    half_cols = w_down.shape[1]
    per_expert = 2
    slot_count = ep_count * per_expert

    in_own = w_gate_up.reshape(width, 2 * half_cols).T
    out_own = w_down.reshape(half_cols, width)
    before, after, low, high = ring_gather(jnp.concatenate([in_own, out_own], axis=0))

    piece_len = gen_cache.size // (per_dev * ep_count)
    flat_cache = (
        gen_cache.reshape(per_dev, ep_count, piece_len)
        .transpose(1, 0, 2)
        .reshape(ep_count, 2, per_dev * piece_len // 2)
    )
    flat_len = flat_cache.shape[2]
    digits = jnp.concatenate([ancestors // 256, ancestors % 256]).astype(jnp.bfloat16)
    side = jnp.pad(digits, (0, 128 - digits.shape[0]))
    flat_cache = jnp.concatenate(
        [flat_cache, jnp.broadcast_to(side, (ep_count, 2, side.shape[0]))], axis=2
    )
    pieces = lax.all_to_all(flat_cache, EP, split_axis=0, concat_axis=0, tiled=True)
    tail = pieces[:, 0, flat_len : flat_len + 2 * per_dev].astype(jnp.int32)
    parents = (tail[:, :per_dev] * 256 + tail[:, per_dev:]).reshape(-1)
    pieces = pieces[:, :, :flat_len].reshape(-1, piece_len)
    chosen = jnp.take(pieces, parents, axis=0, mode="clip").reshape(ep_count, 2, flat_len)
    moved = lax.all_to_all(chosen, EP, split_axis=0, concat_axis=0, tiled=True)
    cache_out = (
        moved.reshape(ep_count, per_dev, piece_len).transpose(1, 0, 2).reshape(gen_cache.shape)
    )
    attn_out = attend(queries, cache_out, new_kv, prompt_cache)

    values_f = tokens_in.astype(jnp.float32).reshape(row_count, width)
    normed = (
        values_f
        * lax.rsqrt(jnp.mean(values_f * values_f, axis=-1, keepdims=True) + 1e-06)
        * norm_gain
    ).astype(jnp.bfloat16)
    rep_place = lax.axis_index("rep")
    own_routes = lax.dynamic_index_in_dim(routes, rep_place, 0, keepdims=False).reshape(
        -1, top_count
    )
    own_gates = lax.dynamic_index_in_dim(gate_weights, rep_place, 0, keepdims=False).reshape(
        -1, top_count
    )
    labels = jnp.pad(own_routes.astype(jnp.bfloat16), ((0, 0), (0, 128 - top_count)))
    blocks = ring_rows(jnp.concatenate([normed, labels], axis=1))
    planes = lax.axis_size("ep_0")
    local = ep_count // planes
    packed = select_rows(lax.axis_index("ep_0"), blocks, width, slot_count)
    rows = lax.all_to_all(
        packed.reshape(local, planes * per_expert, width),
        EP[1:],
        split_axis=0,
        concat_axis=0,
        tiled=True,
    ).reshape(slot_count, width)
    produced = expert(rows, in_own, out_own, before, after, low, high)
    produced = produced.reshape(ep_count, per_expert, width)

    slot_ids = slot_numbers(own_routes, per_expert)
    hits = jnp.arange(slot_count, dtype=jnp.int32)[:, None, None] == slot_ids[None, :, :]
    gate_of_slot = jnp.sum(jnp.where(hits, own_gates[None, :, :], 0.0), axis=-1).T
    came_back = lax.all_to_all(produced, EP, split_axis=0, concat_axis=0, tiled=True)
    came_back = came_back.reshape(slot_count, width)
    summed = jnp.dot(
        gate_of_slot,
        came_back.astype(jnp.float32),
        precision=lax.Precision.HIGHEST,
        preferred_element_type=jnp.float32,
    )
    expert_out = summed.astype(jnp.bfloat16).reshape(per_dev, 2, width)
    return (cache_out, attn_out, expert_out)


def solution(mesh):
    torus = Mesh(mesh.devices.reshape(mesh.shape["rep"], 16, 4, 2), ("rep", "ep_0", "ep_1", "ep_2"))
    placed = (
        P(REP_EP, None, None, None, None),
        P(),
        P(REP_EP),
        P(REP_EP, None, None, None),
        P(REP_EP, None, None, None, None),
        P(REP_EP, None, None),
        P(),
        P(None, EP, None, None),
        P(None, EP, None, None),
        P(EP, None, None, "rep"),
        P(EP, "rep", None),
    )
    return jax.shard_map(
        shards,
        mesh=torus,
        in_specs=placed,
        out_specs=(
            P(REP_EP, None, None, None, None),
            P(REP_EP, None, None, None),
            P(REP_EP, None, None),
        ),
        check_vma=False,
    )
```

```python
import math

import jax
import jax.numpy as jnp
from jax import lax
from jax.experimental import pallas as pl
from jax.experimental.pallas import tpu as pltpu
from jax.sharding import Mesh
from jax.sharding import PartitionSpec as P


EP = ("ep_0", "ep_1", "ep_2")
REP_EP = ("rep", "ep_0", "ep_1", "ep_2")


def shift(block, axis, count, step):
    return lax.ppermute(block, axis, [(i, (i + step) % count) for i in range(count)])


def ring_gather(block):
    half = block.shape[0] // 2
    before = shift(block, "rep", 4, 1)
    after = shift(block, "rep", 4, -1)
    far_low = shift(before[:half], "rep", 4, 1)
    far_high = shift(after[half:], "rep", 4, -1)
    return before, after, far_low, far_high


def ring_rows(block):
    wide = [block] + [shift(block, "ep_0", 16, step) for step in (4, -4, 8)]
    wide = jnp.concatenate(wide, axis=0)
    return [wide] + [shift(wide, "ep_0", 16, step) for step in (1, -1, 2)]


def select_body(place_ref, own_ref, back_ref, ahead_ref, far_ref, out_ref, rows_ref, sems, *, width):
    copies = [
        pltpu.make_async_copy(part, rows_ref.at[n * 64 : (n + 1) * 64], sems.at[n])
        for n, part in enumerate((own_ref, back_ref, ahead_ref, far_ref))
    ]
    for copy in copies:
        copy.start()
    for copy in copies:
        copy.wait()
    count = rows_ref.shape[0]
    slots = out_ref.shape[0]
    place = place_ref[0]
    row = lax.broadcasted_iota(jnp.int32, (count, 1), 0)
    near, wide = row // 64, row // 16 % 4
    distance = jnp.where(near == 1, -1, jnp.where(near == 2, 1, jnp.where(near == 3, -2, 0)))
    distance += jnp.where(wide == 1, -4, jnp.where(wide == 2, 4, jnp.where(wide == 3, -8, 0)))
    source = (place + distance + 16) % 16
    column = lax.broadcasted_iota(jnp.int32, (count, slots), 1)
    expert = place * 8 + column // 32
    ids = rows_ref[:, width:].astype(jnp.int32)
    named = ids[:, 0:1] == expert
    for k in range(1, 8):
        named = named | (ids[:, k : k + 1] == expert)
    lower = lax.broadcasted_iota(jnp.int32, (count, count), 0)
    upper = lax.broadcasted_iota(jnp.int32, (count, count), 1)
    earlier = (upper < lower) & (upper // 16 == lower // 16)
    rank = jnp.dot(
        earlier.astype(jnp.float32).astype(jnp.bfloat16),
        named.astype(jnp.float32).astype(jnp.bfloat16),
        preferred_element_type=jnp.float32,
    ).astype(jnp.int32)
    chosen = named & (source * 2 + rank == column % 32)
    out_ref[...] = lax.dot_general(
        chosen.astype(jnp.float32).astype(jnp.bfloat16),
        rows_ref[:, :width],
        (((0,), (0,)), ((), ())),
        preferred_element_type=jnp.float32,
    ).astype(jnp.bfloat16)


def select_rows(place, blocks, width, slots):
    rows = sum(b.shape[0] for b in blocks)
    return pl.pallas_call(
        lambda *refs: select_body(*refs, width=width),
        out_shape=jax.ShapeDtypeStruct((slots, width), jnp.bfloat16),
        in_specs=[pl.BlockSpec(memory_space=pltpu.SMEM)]
        + [pl.BlockSpec(memory_space=pl.ANY)] * 4,
        out_specs=pl.BlockSpec(memory_space=pltpu.VMEM),
        scratch_shapes=[
            pltpu.VMEM((rows, blocks[0].shape[1]), jnp.bfloat16),
            pltpu.SemaphoreType.DMA((4,)),
        ],
        name="select_rows",
    )(place.reshape(1), *blocks)


def expert_body(
    rows_hbm, own_hbm, before_hbm, after_hbm, low_hbm, high_hbm, result_hbm,
    rows, own, before, after, far, result, sems,
):
    hidden = own.shape[0] // 3
    half = low_hbm.shape[0]
    copies = [
        pltpu.make_async_copy(src, dst, sems.at[n])
        for n, (src, dst) in enumerate(
            (
                (rows_hbm, rows),
                (own_hbm, own),
                (before_hbm, before),
                (after_hbm, after),
                (low_hbm, far.at[:half]),
                (high_hbm, far.at[half:]),
            )
        )
    ]
    for copy in copies:
        copy.start()
    count = rows.shape[0]
    to = lax.broadcasted_iota(jnp.int32, (count, count), 0)
    come = lax.broadcasted_iota(jnp.int32, (count, count), 1)
    order = come == to // 2 % 8 * 32 + to // 16 * 2 + to % 2
    order = order.astype(jnp.float32).astype(jnp.bfloat16)
    total = None
    contract = (((1,), (1,)), ((), ()))
    for weights, waits in ((own, (0, 1)), (before, (2,)), (after, (3,)), (far, (4, 5))):
        for n in waits:
            copies[n].wait()
        both = lax.dot_general(
            rows[...], weights[: 2 * hidden], contract, preferred_element_type=jnp.float32
        )
        gate, upward = both[:, :hidden], both[:, hidden:]
        act = (gate / (1.0 + jnp.exp(-gate)) * upward).astype(jnp.bfloat16)
        act = jnp.dot(order, act, preferred_element_type=jnp.float32).astype(jnp.bfloat16)
        part = jnp.dot(act, weights[2 * hidden :], preferred_element_type=jnp.float32)
        total = part if total is None else total + part
    result[...] = total.astype(jnp.bfloat16).reshape(result.shape)
    last = pltpu.make_async_copy(result, result_hbm, sems.at[6])
    last.start()
    last.wait()


def expert(rows, own, before, after, low, high):
    count, width = rows.shape
    return pl.pallas_call(
        expert_body,
        out_shape=jax.ShapeDtypeStruct((count // 2, 2, width), jnp.bfloat16),
        in_specs=[pl.BlockSpec(memory_space=pl.ANY)] + [pl.BlockSpec(memory_space=pltpu.HBM)] * 5,
        out_specs=pl.BlockSpec(memory_space=pltpu.HBM),
        scratch_shapes=[pltpu.VMEM((count, width), jnp.bfloat16)]
        + [pltpu.VMEM(own.shape, jnp.bfloat16)] * 4
        + [pltpu.VMEM((count // 2, 2, width), jnp.bfloat16), pltpu.SemaphoreType.DMA((7,))],
        compiler_params=pltpu.CompilerParams(vmem_limit_bytes=32 * 1024 * 1024),
        name="expert",
    )(rows, own, before, after, low, high)


def attend(queries, gen_block, new_block, prompt_cache):
    count = queries.shape[0]
    heads = queries.shape[2]
    head_dim = queries.shape[3]
    kv_heads = new_block.shape[3]
    score_scale = 1.0 / math.sqrt(head_dim)
    grouped = queries.reshape(count, 2, kv_heads, heads // kv_heads, head_dim)
    prompt_scores = (
        jnp.einsum(
            "btngd,snd->btngs", grouped, prompt_cache[:, 0], preferred_element_type=jnp.float32
        )
        * score_scale
    )
    gen_scores = (
        jnp.einsum(
            "btngd,bsnd->btngs", grouped, gen_block[:, :, 0], preferred_element_type=jnp.float32
        )
        * score_scale
    )
    new_scores = (
        jnp.einsum(
            "btngd,bsnd->btngs", grouped, new_block[:, :, 0], preferred_element_type=jnp.float32
        )
        * score_scale
    )
    causal = lax.broadcasted_iota(jnp.int32, (2, 2), 1) <= lax.broadcasted_iota(
        jnp.int32, (2, 2), 0
    )
    new_scores = jnp.where(causal[None, :, None, None, :], new_scores, -jnp.inf)
    row_max = jnp.maximum(
        jnp.maximum(prompt_scores.max(-1), gen_scores.max(-1)), new_scores.max(-1)
    )[..., None]
    prompt_exp = jnp.exp(prompt_scores - row_max)
    gen_exp = jnp.exp(gen_scores - row_max)
    new_exp = jnp.exp(new_scores - row_max)
    denom = (prompt_exp.sum(-1) + gen_exp.sum(-1) + new_exp.sum(-1))[..., None]
    prompt_weights = (prompt_exp / denom).astype(jnp.bfloat16)
    gen_weights = (gen_exp / denom).astype(jnp.bfloat16)
    new_weights = (new_exp / denom).astype(jnp.bfloat16)
    result = jnp.einsum(
        "btngs,snd->btngd", prompt_weights, prompt_cache[:, 1], preferred_element_type=jnp.float32
    )
    result = result + jnp.einsum(
        "btngs,bsnd->btngd", gen_weights, gen_block[:, :, 1], preferred_element_type=jnp.float32
    )
    result = result + jnp.einsum(
        "btngs,bsnd->btngd", new_weights, new_block[:, :, 1], preferred_element_type=jnp.float32
    )
    return result.reshape(count, 2, heads, head_dim).astype(jnp.bfloat16)


def slot_numbers(expert_ids, capacity):
    flat_ids = expert_ids.reshape(-1)
    count = flat_ids.shape[0]
    earlier = lax.broadcasted_iota(jnp.int32, (count, count), 1) < lax.broadcasted_iota(
        jnp.int32, (count, count), 0
    )
    same = (flat_ids[:, None] == flat_ids[None, :]) & earlier
    rank = jnp.sum(same.astype(jnp.int32), axis=1)
    return (flat_ids * capacity + rank).reshape(expert_ids.shape)


def shards(
    gen_cache,
    prompt_cache,
    ancestors,
    queries,
    new_kv,
    tokens_in,
    norm_gain,
    routes,
    gate_weights,
    w_gate_up,
    w_down,
):
    ep_count = lax.axis_size(EP)
    per_dev = gen_cache.shape[0]
    row_count = 2 * per_dev
    width = tokens_in.shape[2]
    top_count = routes.shape[3]
    half_cols = w_down.shape[1]
    per_expert = 2
    slot_count = ep_count * per_expert

    in_own = w_gate_up.reshape(width, 2 * half_cols).T
    out_own = w_down.reshape(half_cols, width)
    own = jnp.concatenate([in_own, out_own], axis=0)
    before, after, low, high = ring_gather(own)

    piece_len = gen_cache.size // (per_dev * ep_count)
    flat_cache = (
        gen_cache.reshape(per_dev, ep_count, piece_len)
        .transpose(1, 0, 2)
        .reshape(ep_count, 2, per_dev * piece_len // 2)
    )
    flat_len = flat_cache.shape[2]
    digits = jnp.concatenate([ancestors // 256, ancestors % 256]).astype(jnp.bfloat16)
    side = jnp.pad(digits, (0, 128 - digits.shape[0]))
    flat_cache = jnp.concatenate(
        [flat_cache, jnp.broadcast_to(side, (ep_count, 2, side.shape[0]))], axis=2
    )
    pieces = lax.all_to_all(flat_cache, EP, split_axis=0, concat_axis=0, tiled=True)
    tail = pieces[:, 0, flat_len : flat_len + 2 * per_dev].astype(jnp.int32)
    parents = (tail[:, :per_dev] * 256 + tail[:, per_dev:]).reshape(-1)
    pieces = pieces[:, :, :flat_len].reshape(-1, piece_len)
    chosen = jnp.take(pieces, parents, axis=0, mode="clip").reshape(ep_count, 2, flat_len)
    moved = lax.all_to_all(chosen, EP, split_axis=0, concat_axis=0, tiled=True)
    cache_out = (
        moved.reshape(ep_count, per_dev, piece_len).transpose(1, 0, 2).reshape(gen_cache.shape)
    )
    attn_out = attend(queries, cache_out, new_kv, prompt_cache)

    values_f = tokens_in.astype(jnp.float32).reshape(row_count, width)
    normed = (
        values_f
        * lax.rsqrt(jnp.mean(values_f * values_f, axis=-1, keepdims=True) + 1e-06)
        * norm_gain
    ).astype(jnp.bfloat16)
    rep_place = lax.axis_index("rep")
    own_routes = lax.dynamic_index_in_dim(routes, rep_place, 0, keepdims=False).reshape(
        -1, top_count
    )
    own_gates = lax.dynamic_index_in_dim(gate_weights, rep_place, 0, keepdims=False).reshape(
        -1, top_count
    )
    labels = jnp.pad(own_routes.astype(jnp.bfloat16), ((0, 0), (0, 128 - top_count)))
    blocks = ring_rows(jnp.concatenate([normed, labels], axis=1))
    planes = lax.axis_size("ep_0")
    local = ep_count // planes
    packed = select_rows(lax.axis_index("ep_0"), blocks, width, slot_count)
    rows = lax.all_to_all(
        packed.reshape(local, planes * per_expert, width),
        EP[1:],
        split_axis=0,
        concat_axis=0,
        tiled=True,
    ).reshape(slot_count, width)
    produced = expert(rows, own, before, after, low, high)

    slot_ids = slot_numbers(own_routes, per_expert)
    hits = jnp.arange(slot_count, dtype=jnp.int32)[:, None, None] == slot_ids[None, :, :]
    gate_of_slot = jnp.sum(jnp.where(hits, own_gates[None, :, :], 0.0), axis=-1).T
    came_back = lax.all_to_all(produced, EP, split_axis=0, concat_axis=0, tiled=True)
    came_back = came_back.reshape(slot_count, width)
    summed = jnp.dot(
        gate_of_slot,
        came_back.astype(jnp.float32),
        precision=lax.Precision.HIGHEST,
        preferred_element_type=jnp.float32,
    )
    expert_out = summed.astype(jnp.bfloat16).reshape(per_dev, 2, width)
    return (cache_out, attn_out, expert_out)


def solution(mesh):
    torus = Mesh(mesh.devices.reshape(mesh.shape["rep"], 16, 4, 2), ("rep", "ep_0", "ep_1", "ep_2"))
    placed = (
        P(REP_EP, None, None, None, None),
        P(),
        P(REP_EP),
        P(REP_EP, None, None, None),
        P(REP_EP, None, None, None, None),
        P(REP_EP, None, None),
        P(),
        P(None, EP, None, None),
        P(None, EP, None, None),
        P(EP, None, None, "rep"),
        P(EP, "rep", None),
    )
    return jax.shard_map(
        shards,
        mesh=torus,
        in_specs=placed,
        out_specs=(
            P(REP_EP, None, None, None, None),
            P(REP_EP, None, None, None),
            P(REP_EP, None, None),
        ),
        check_vma=False,
    )
```

```python
import math

import jax
import jax.numpy as jnp
from jax import lax
from jax.experimental import pallas as pl
from jax.experimental.pallas import tpu as pltpu
from jax.sharding import Mesh
from jax.sharding import PartitionSpec as P


EP = ("wide", "near", "ep_1", "ep_2")
REP_EP = ("rep",) + EP
PLANES = EP[:2]


def shift(block, axis, count, step):
    return lax.ppermute(block, axis, [(i, (i + step) % count) for i in range(count)])


def ring_gather(block):
    half = block.shape[0] // 2
    before = shift(block, "rep", 4, 1)
    after = shift(block, "rep", 4, -1)
    far_low = shift(before[:half], "rep", 4, 1)
    far_high = shift(after[half:], "rep", 4, -1)
    return before, after, far_low, far_high


def ring_rows(block):
    wide = lax.all_gather(block, "wide", axis=0, tiled=True)
    return [wide] + [shift(wide, PLANES, 16, step) for step in (1, -1, 2)]


def select_body(place_ref, own_ref, back_ref, ahead_ref, far_ref, out_ref, rows_ref, sems, *, width):
    copies = [
        pltpu.make_async_copy(part, rows_ref.at[n * 64 : (n + 1) * 64], sems.at[n])
        for n, part in enumerate((own_ref, back_ref, ahead_ref, far_ref))
    ]
    for copy in copies:
        copy.start()
    for copy in copies:
        copy.wait()
    count = rows_ref.shape[0]
    slots = out_ref.shape[0]
    place = place_ref[0]
    row = lax.broadcasted_iota(jnp.int32, (count, 1), 0)
    near, wide = row // 64, row // 16 % 4
    distance = jnp.where(near == 1, -1, jnp.where(near == 2, 1, jnp.where(near == 3, -2, 0)))
    source = wide * 4 + (place + distance + 16) % 4
    column = lax.broadcasted_iota(jnp.int32, (count, slots), 1)
    expert = place * 8 + column // 32
    ids = rows_ref[:, width:].astype(jnp.int32)
    named = ids[:, 0:1] == expert
    for k in range(1, 8):
        named = named | (ids[:, k : k + 1] == expert)
    lower = lax.broadcasted_iota(jnp.int32, (count, count), 0)
    upper = lax.broadcasted_iota(jnp.int32, (count, count), 1)
    earlier = (upper < lower) & (upper // 16 == lower // 16)
    rank = jnp.dot(
        earlier.astype(jnp.float32).astype(jnp.bfloat16),
        named.astype(jnp.float32).astype(jnp.bfloat16),
        preferred_element_type=jnp.float32,
    ).astype(jnp.int32)
    chosen = named & (source * 2 + rank == column % 32)
    out_ref[...] = lax.dot_general(
        chosen.astype(jnp.float32).astype(jnp.bfloat16),
        rows_ref[:, :width],
        (((0,), (0,)), ((), ())),
        preferred_element_type=jnp.float32,
    ).astype(jnp.bfloat16)


def select_rows(place, blocks, width, slots):
    rows = sum(b.shape[0] for b in blocks)
    return pl.pallas_call(
        lambda *refs: select_body(*refs, width=width),
        out_shape=jax.ShapeDtypeStruct((slots, width), jnp.bfloat16),
        in_specs=[pl.BlockSpec(memory_space=pltpu.SMEM)]
        + [pl.BlockSpec(memory_space=pl.ANY)] * 4,
        out_specs=pl.BlockSpec(memory_space=pltpu.VMEM),
        scratch_shapes=[
            pltpu.VMEM((rows, blocks[0].shape[1]), jnp.bfloat16),
            pltpu.SemaphoreType.DMA((4,)),
        ],
        name="select_rows",
    )(place.reshape(1), *blocks)


def expert_body(
    rows_hbm, own_hbm, before_hbm, after_hbm, low_hbm, high_hbm, result_hbm,
    rows, own, before, after, far, result, sems,
):
    hidden = own.shape[0] // 3
    half = low_hbm.shape[0]
    copies = [
        pltpu.make_async_copy(src, dst, sems.at[n])
        for n, (src, dst) in enumerate(
            (
                (rows_hbm, rows),
                (own_hbm, own),
                (before_hbm, before),
                (after_hbm, after),
                (low_hbm, far.at[:half]),
                (high_hbm, far.at[half:]),
            )
        )
    ]
    for copy in copies:
        copy.start()
    count = rows.shape[0]
    to = lax.broadcasted_iota(jnp.int32, (count, count), 0)
    come = lax.broadcasted_iota(jnp.int32, (count, count), 1)
    order = come == to // 2 % 8 * 32 + to // 16 * 2 + to % 2
    order = order.astype(jnp.float32).astype(jnp.bfloat16)
    total = None
    contract = (((1,), (1,)), ((), ()))
    for weights, waits in ((own, (0, 1)), (before, (2,)), (after, (3,)), (far, (4, 5))):
        for n in waits:
            copies[n].wait()
        both = lax.dot_general(
            rows[...], weights[: 2 * hidden], contract, preferred_element_type=jnp.float32
        )
        gate, upward = both[:, :hidden], both[:, hidden:]
        act = (gate / (1.0 + jnp.exp(-gate)) * upward).astype(jnp.bfloat16)
        act = jnp.dot(order, act, preferred_element_type=jnp.float32).astype(jnp.bfloat16)
        part = jnp.dot(act, weights[2 * hidden :], preferred_element_type=jnp.float32)
        total = part if total is None else total + part
    result[...] = total.astype(jnp.bfloat16).reshape(result.shape)
    last = pltpu.make_async_copy(result, result_hbm, sems.at[6])
    last.start()
    last.wait()


def expert(rows, own, before, after, low, high):
    count, width = rows.shape
    return pl.pallas_call(
        expert_body,
        out_shape=jax.ShapeDtypeStruct((count // 2, 2, width), jnp.bfloat16),
        in_specs=[pl.BlockSpec(memory_space=pl.ANY)] + [pl.BlockSpec(memory_space=pltpu.HBM)] * 5,
        out_specs=pl.BlockSpec(memory_space=pltpu.HBM),
        scratch_shapes=[pltpu.VMEM((count, width), jnp.bfloat16)]
        + [pltpu.VMEM(own.shape, jnp.bfloat16)] * 4
        + [pltpu.VMEM((count // 2, 2, width), jnp.bfloat16), pltpu.SemaphoreType.DMA((7,))],
        compiler_params=pltpu.CompilerParams(vmem_limit_bytes=32 * 1024 * 1024),
        name="expert",
    )(rows, own, before, after, low, high)


def resample_body(pieces_any, out_ref, pieces_ref, sem):
    copy = pltpu.make_async_copy(pieces_any, pieces_ref, sem)
    copy.start()
    copy.wait()
    devices, two, width = pieces_ref.shape
    count, length = devices * two, out_ref.shape[2]
    rows = pieces_ref[...].reshape(count, width)
    digits = rows[:, length : length + 8].astype(jnp.float32).astype(jnp.int32)
    parents = digits[:, :4] * 256 + digits[:, 4:]
    piece = length // 4
    stacked = jnp.concatenate([rows[:, m * piece : (m + 1) * piece] for m in range(4)], axis=0)
    column = lax.broadcasted_iota(jnp.int32, (count, 4 * count), 1)
    particle = column % count * 4 + column // count
    chosen = []
    for m in range(4):
        onehot = (parents[:, m : m + 1] == particle).astype(jnp.float32).astype(jnp.bfloat16)
        picked = jnp.dot(onehot, stacked, preferred_element_type=jnp.float32)
        chosen.append(picked.astype(jnp.bfloat16))
    out_ref[...] = jnp.concatenate(chosen, axis=1).reshape(out_ref.shape)


def resample(pieces, length):
    return pl.pallas_call(
        resample_body,
        out_shape=jax.ShapeDtypeStruct(pieces.shape[:2] + (length,), jnp.bfloat16),
        in_specs=[pl.BlockSpec(memory_space=pl.ANY)],
        out_specs=pl.BlockSpec(memory_space=pltpu.VMEM),
        scratch_shapes=[pltpu.VMEM(pieces.shape, jnp.bfloat16), pltpu.SemaphoreType.DMA(())],
        name="resample",
    )(pieces)


def attend(queries, gen_block, new_block, prompt_cache):
    count = queries.shape[0]
    heads = queries.shape[2]
    head_dim = queries.shape[3]
    kv_heads = new_block.shape[3]
    score_scale = 1.0 / math.sqrt(head_dim)
    grouped = queries.reshape(count, 2, kv_heads, heads // kv_heads, head_dim)
    prompt_scores = (
        jnp.einsum(
            "btngd,snd->btngs", grouped, prompt_cache[:, 0], preferred_element_type=jnp.float32
        )
        * score_scale
    )
    gen_scores = (
        jnp.einsum(
            "btngd,bsnd->btngs", grouped, gen_block[:, :, 0], preferred_element_type=jnp.float32
        )
        * score_scale
    )
    new_scores = (
        jnp.einsum(
            "btngd,bsnd->btngs", grouped, new_block[:, :, 0], preferred_element_type=jnp.float32
        )
        * score_scale
    )
    causal = lax.broadcasted_iota(jnp.int32, (2, 2), 1) <= lax.broadcasted_iota(
        jnp.int32, (2, 2), 0
    )
    new_scores = jnp.where(causal[None, :, None, None, :], new_scores, -jnp.inf)
    row_max = jnp.maximum(
        jnp.maximum(prompt_scores.max(-1), gen_scores.max(-1)), new_scores.max(-1)
    )[..., None]
    prompt_exp = jnp.exp(prompt_scores - row_max)
    gen_exp = jnp.exp(gen_scores - row_max)
    new_exp = jnp.exp(new_scores - row_max)
    denom = (prompt_exp.sum(-1) + gen_exp.sum(-1) + new_exp.sum(-1))[..., None]
    prompt_weights = (prompt_exp / denom).astype(jnp.bfloat16)
    gen_weights = (gen_exp / denom).astype(jnp.bfloat16)
    new_weights = (new_exp / denom).astype(jnp.bfloat16)
    result = jnp.einsum(
        "btngs,snd->btngd", prompt_weights, prompt_cache[:, 1], preferred_element_type=jnp.float32
    )
    result = result + jnp.einsum(
        "btngs,bsnd->btngd", gen_weights, gen_block[:, :, 1], preferred_element_type=jnp.float32
    )
    result = result + jnp.einsum(
        "btngs,bsnd->btngd", new_weights, new_block[:, :, 1], preferred_element_type=jnp.float32
    )
    return result.reshape(count, 2, heads, head_dim).astype(jnp.bfloat16)


def slot_numbers(expert_ids, capacity):
    flat_ids = expert_ids.reshape(-1)
    count = flat_ids.shape[0]
    earlier = lax.broadcasted_iota(jnp.int32, (count, count), 1) < lax.broadcasted_iota(
        jnp.int32, (count, count), 0
    )
    same = (flat_ids[:, None] == flat_ids[None, :]) & earlier
    rank = jnp.sum(same.astype(jnp.int32), axis=1)
    return (flat_ids * capacity + rank).reshape(expert_ids.shape)


def shards(
    gen_cache,
    prompt_cache,
    ancestors,
    queries,
    new_kv,
    tokens_in,
    norm_gain,
    routes,
    gate_weights,
    w_gate_up,
    w_down,
):
    ep_count = lax.axis_size(EP)
    per_dev = gen_cache.shape[0]
    row_count = 2 * per_dev
    width = tokens_in.shape[2]
    top_count = routes.shape[3]
    half_cols = w_down.shape[1]
    per_expert = 2
    slot_count = ep_count * per_expert

    in_own = w_gate_up.reshape(width, 2 * half_cols).T
    out_own = w_down.reshape(half_cols, width)
    own = jnp.concatenate([in_own, out_own], axis=0)
    before, after, low, high = ring_gather(own)

    piece_len = gen_cache.size // (per_dev * ep_count)
    flat_cache = (
        gen_cache.reshape(per_dev, ep_count, piece_len)
        .transpose(1, 0, 2)
        .reshape(ep_count, 2, per_dev * piece_len // 2)
    )
    flat_len = flat_cache.shape[2]
    fours = ancestors.reshape(2, per_dev // 2)
    digits = jnp.concatenate([fours // 256, fours % 256], axis=1).astype(jnp.bfloat16)
    side = jnp.pad(digits, ((0, 0), (0, 128 - digits.shape[1])))
    flat_cache = jnp.concatenate(
        [flat_cache, jnp.broadcast_to(side, (ep_count,) + side.shape)], axis=2
    )
    pieces = lax.all_to_all(flat_cache, EP, split_axis=0, concat_axis=0, tiled=True)
    chosen = resample(pieces, flat_len)
    moved = lax.all_to_all(chosen, EP, split_axis=0, concat_axis=0, tiled=True)
    cache_out = (
        moved.reshape(ep_count, per_dev, piece_len).transpose(1, 0, 2).reshape(gen_cache.shape)
    )
    attn_out = attend(queries, cache_out, new_kv, prompt_cache)

    values_f = tokens_in.astype(jnp.float32).reshape(row_count, width)
    normed = (
        values_f
        * lax.rsqrt(jnp.mean(values_f * values_f, axis=-1, keepdims=True) + 1e-06)
        * norm_gain
    ).astype(jnp.bfloat16)
    rep_place = lax.axis_index("rep")
    own_routes = lax.dynamic_index_in_dim(routes, rep_place, 0, keepdims=False).reshape(
        -1, top_count
    )
    own_gates = lax.dynamic_index_in_dim(gate_weights, rep_place, 0, keepdims=False).reshape(
        -1, top_count
    )
    labels = jnp.pad(own_routes.astype(jnp.bfloat16), ((0, 0), (0, 128 - top_count)))
    blocks = ring_rows(jnp.concatenate([normed, labels], axis=1))
    planes = lax.axis_size(PLANES)
    local = ep_count // planes
    packed = select_rows(lax.axis_index(PLANES), blocks, width, slot_count)
    rows = lax.all_to_all(
        packed.reshape(local, planes * per_expert, width),
        EP[2:],
        split_axis=0,
        concat_axis=0,
        tiled=True,
    ).reshape(slot_count, width)
    produced = expert(rows, own, before, after, low, high)

    slot_ids = slot_numbers(own_routes, per_expert)
    hits = jnp.arange(slot_count, dtype=jnp.int32)[:, None, None] == slot_ids[None, :, :]
    gate_of_slot = jnp.sum(jnp.where(hits, own_gates[None, :, :], 0.0), axis=-1).T
    came_back = lax.all_to_all(produced, EP, split_axis=0, concat_axis=0, tiled=True)
    came_back = came_back.reshape(slot_count, width)
    summed = jnp.dot(
        gate_of_slot,
        came_back.astype(jnp.float32),
        precision=lax.Precision.HIGHEST,
        preferred_element_type=jnp.float32,
    )
    expert_out = summed.astype(jnp.bfloat16).reshape(per_dev, 2, width)
    return (cache_out, attn_out, expert_out)


def solution(mesh):
    torus = Mesh(mesh.devices.reshape(mesh.shape["rep"], 4, 4, 4, 2), REP_EP)
    placed = (
        P(REP_EP, None, None, None, None),
        P(),
        P(REP_EP),
        P(REP_EP, None, None, None),
        P(REP_EP, None, None, None, None),
        P(REP_EP, None, None),
        P(),
        P(None, EP, None, None),
        P(None, EP, None, None),
        P(EP, None, None, "rep"),
        P(EP, "rep", None),
    )
    return jax.shard_map(
        shards,
        mesh=torus,
        in_specs=placed,
        out_specs=(
            P(REP_EP, None, None, None, None),
            P(REP_EP, None, None, None),
            P(REP_EP, None, None),
        ),
        check_vma=False,
    )
```

```python
import math

import jax
import jax.numpy as jnp
from jax import lax
from jax.experimental import pallas as pl
from jax.experimental.pallas import tpu as pltpu
from jax.sharding import Mesh
from jax.sharding import PartitionSpec as P


EP = ("wide", "near", "ep_1", "ep_2")
REP_EP = ("rep",) + EP
PLANES = EP[:2]


def shift(block, axis, count, step):
    return lax.ppermute(block, axis, [(i, (i + step) % count) for i in range(count)])


def ring_gather(block):
    half = block.shape[0] // 2
    before = shift(block, "rep", 4, 1)
    after = shift(block, "rep", 4, -1)
    far_low = shift(before[:half], "rep", 4, 1)
    far_high = shift(after[half:], "rep", 4, -1)
    return before, after, far_low, far_high


def ring_rows(block):
    wide = [block] + [shift(block, PLANES, 16, step) for step in (4, -4, 8)]
    wide = jnp.concatenate(wide, axis=0)
    return [wide] + [shift(wide, PLANES, 16, step) for step in (1, -1, 2)]


def select_body(place_ref, own_ref, back_ref, ahead_ref, far_ref, out_ref, rows_ref, sems, *, width):
    copies = [
        pltpu.make_async_copy(part, rows_ref.at[n * 64 : (n + 1) * 64], sems.at[n])
        for n, part in enumerate((own_ref, back_ref, ahead_ref, far_ref))
    ]
    for copy in copies:
        copy.start()
    for copy in copies:
        copy.wait()
    count = rows_ref.shape[0]
    slots = out_ref.shape[0]
    place = place_ref[0]
    row = lax.broadcasted_iota(jnp.int32, (count, 1), 0)
    near, wide = row // 64, row // 16 % 4
    distance = jnp.where(near == 1, -1, jnp.where(near == 2, 1, jnp.where(near == 3, -2, 0)))
    distance += jnp.where(wide == 1, -4, jnp.where(wide == 2, 4, jnp.where(wide == 3, -8, 0)))
    source = (place + distance + 16) % 16
    column = lax.broadcasted_iota(jnp.int32, (count, slots), 1)
    expert = place * 8 + column // 32
    ids = rows_ref[:, width:].astype(jnp.int32)
    named = ids[:, 0:1] == expert
    for k in range(1, 8):
        named = named | (ids[:, k : k + 1] == expert)
    lower = lax.broadcasted_iota(jnp.int32, (count, count), 0)
    upper = lax.broadcasted_iota(jnp.int32, (count, count), 1)
    earlier = (upper < lower) & (upper // 16 == lower // 16)
    rank = jnp.dot(
        earlier.astype(jnp.float32).astype(jnp.bfloat16),
        named.astype(jnp.float32).astype(jnp.bfloat16),
        preferred_element_type=jnp.float32,
    ).astype(jnp.int32)
    chosen = named & (source * 2 + rank == column % 32)
    out_ref[...] = lax.dot_general(
        chosen.astype(jnp.float32).astype(jnp.bfloat16),
        rows_ref[:, :width],
        (((0,), (0,)), ((), ())),
        preferred_element_type=jnp.float32,
    ).astype(jnp.bfloat16)


def select_rows(place, blocks, width, slots):
    rows = sum(b.shape[0] for b in blocks)
    return pl.pallas_call(
        lambda *refs: select_body(*refs, width=width),
        out_shape=jax.ShapeDtypeStruct((slots, width), jnp.bfloat16),
        in_specs=[pl.BlockSpec(memory_space=pltpu.SMEM)]
        + [pl.BlockSpec(memory_space=pl.ANY)] * 4,
        out_specs=pl.BlockSpec(memory_space=pltpu.VMEM),
        scratch_shapes=[
            pltpu.VMEM((rows, blocks[0].shape[1]), jnp.bfloat16),
            pltpu.SemaphoreType.DMA((4,)),
        ],
        name="select_rows",
    )(place.reshape(1), *blocks)


def expert_body(
    rows_hbm, own_hbm, before_hbm, after_hbm, low_hbm, high_hbm, result,
    rows, own, before, after, far, sems,
):
    hidden = own.shape[0] // 3
    half = low_hbm.shape[0]
    copies = [
        pltpu.make_async_copy(src, dst, sems.at[n])
        for n, (src, dst) in enumerate(
            (
                (rows_hbm, rows),
                (own_hbm, own),
                (before_hbm, before),
                (after_hbm, after),
                (low_hbm, far.at[:half]),
                (high_hbm, far.at[half:]),
            )
        )
    ]
    for copy in copies:
        copy.start()
    count = rows.shape[0]
    to = lax.broadcasted_iota(jnp.int32, (count, count), 0)
    come = lax.broadcasted_iota(jnp.int32, (count, count), 1)
    order = come == to // 2 % 8 * 32 + to // 16 * 2 + to % 2
    order = order.astype(jnp.float32).astype(jnp.bfloat16)
    total = None
    contract = (((1,), (1,)), ((), ()))
    for weights, waits in ((own, (0, 1)), (before, (2,)), (after, (3,)), (far, (4, 5))):
        for n in waits:
            copies[n].wait()
        both = lax.dot_general(
            rows[...], weights[: 2 * hidden], contract, preferred_element_type=jnp.float32
        )
        gate, upward = both[:, :hidden], both[:, hidden:]
        act = (gate / (1.0 + jnp.exp(-gate)) * upward).astype(jnp.bfloat16)
        act = jnp.dot(order, act, preferred_element_type=jnp.float32).astype(jnp.bfloat16)
        part = jnp.dot(act, weights[2 * hidden :], preferred_element_type=jnp.float32)
        total = part if total is None else total + part
    result[...] = total.astype(jnp.bfloat16).reshape(result.shape)


def expert(rows, own, before, after, low, high):
    count, width = rows.shape
    return pl.pallas_call(
        expert_body,
        out_shape=jax.ShapeDtypeStruct((count // 2, 2, width), jnp.bfloat16),
        in_specs=[pl.BlockSpec(memory_space=pl.ANY)] + [pl.BlockSpec(memory_space=pltpu.HBM)] * 5,
        out_specs=pl.BlockSpec(memory_space=pltpu.VMEM),
        scratch_shapes=[pltpu.VMEM((count, width), jnp.bfloat16)]
        + [pltpu.VMEM(own.shape, jnp.bfloat16)] * 4
        + [pltpu.SemaphoreType.DMA((6,))],
        compiler_params=pltpu.CompilerParams(vmem_limit_bytes=32 * 1024 * 1024),
        name="expert",
    )(rows, own, before, after, low, high)


def resample_body(pieces_any, out_ref, pieces_ref, sem):
    copy = pltpu.make_async_copy(pieces_any, pieces_ref, sem)
    copy.start()
    copy.wait()
    devices, two, width = pieces_ref.shape
    count, length = devices * two, out_ref.shape[2]
    rows = pieces_ref[...].reshape(count, width)
    digits = rows[:, length : length + 8].astype(jnp.float32).astype(jnp.int32)
    parents = digits[:, :4] * 256 + digits[:, 4:]
    piece = length // 4
    stacked = jnp.concatenate([rows[:, m * piece : (m + 1) * piece] for m in range(4)], axis=0)
    column = lax.broadcasted_iota(jnp.int32, (count, 4 * count), 1)
    particle = column % count * 4 + column // count
    chosen = []
    for m in range(4):
        onehot = (parents[:, m : m + 1] == particle).astype(jnp.float32).astype(jnp.bfloat16)
        picked = jnp.dot(onehot, stacked, preferred_element_type=jnp.float32)
        chosen.append(picked.astype(jnp.bfloat16))
    out_ref[...] = jnp.concatenate(chosen, axis=1).reshape(out_ref.shape)


def resample(pieces, length):
    return pl.pallas_call(
        resample_body,
        out_shape=jax.ShapeDtypeStruct(pieces.shape[:2] + (length,), jnp.bfloat16),
        in_specs=[pl.BlockSpec(memory_space=pl.ANY)],
        out_specs=pl.BlockSpec(memory_space=pltpu.VMEM),
        scratch_shapes=[pltpu.VMEM(pieces.shape, jnp.bfloat16), pltpu.SemaphoreType.DMA(())],
        name="resample",
    )(pieces)


def attend(queries, gen_block, new_block, prompt_cache):
    count = queries.shape[0]
    heads = queries.shape[2]
    head_dim = queries.shape[3]
    kv_heads = new_block.shape[3]
    score_scale = 1.0 / math.sqrt(head_dim)
    grouped = queries.reshape(count, 2, kv_heads, heads // kv_heads, head_dim)
    prompt_scores = (
        jnp.einsum(
            "btngd,snd->btngs", grouped, prompt_cache[:, 0], preferred_element_type=jnp.float32
        )
        * score_scale
    )
    gen_scores = (
        jnp.einsum(
            "btngd,bsnd->btngs", grouped, gen_block[:, :, 0], preferred_element_type=jnp.float32
        )
        * score_scale
    )
    new_scores = (
        jnp.einsum(
            "btngd,bsnd->btngs", grouped, new_block[:, :, 0], preferred_element_type=jnp.float32
        )
        * score_scale
    )
    causal = lax.broadcasted_iota(jnp.int32, (2, 2), 1) <= lax.broadcasted_iota(
        jnp.int32, (2, 2), 0
    )
    new_scores = jnp.where(causal[None, :, None, None, :], new_scores, -jnp.inf)
    row_max = jnp.maximum(
        jnp.maximum(prompt_scores.max(-1), gen_scores.max(-1)), new_scores.max(-1)
    )[..., None]
    prompt_exp = jnp.exp(prompt_scores - row_max)
    gen_exp = jnp.exp(gen_scores - row_max)
    new_exp = jnp.exp(new_scores - row_max)
    denom = (prompt_exp.sum(-1) + gen_exp.sum(-1) + new_exp.sum(-1))[..., None]
    prompt_weights = (prompt_exp / denom).astype(jnp.bfloat16)
    gen_weights = (gen_exp / denom).astype(jnp.bfloat16)
    new_weights = (new_exp / denom).astype(jnp.bfloat16)
    result = jnp.einsum(
        "btngs,snd->btngd", prompt_weights, prompt_cache[:, 1], preferred_element_type=jnp.float32
    )
    result = result + jnp.einsum(
        "btngs,bsnd->btngd", gen_weights, gen_block[:, :, 1], preferred_element_type=jnp.float32
    )
    result = result + jnp.einsum(
        "btngs,bsnd->btngd", new_weights, new_block[:, :, 1], preferred_element_type=jnp.float32
    )
    return result.reshape(count, 2, heads, head_dim).astype(jnp.bfloat16)


def slot_numbers(expert_ids, capacity):
    flat_ids = expert_ids.reshape(-1)
    count = flat_ids.shape[0]
    earlier = lax.broadcasted_iota(jnp.int32, (count, count), 1) < lax.broadcasted_iota(
        jnp.int32, (count, count), 0
    )
    same = (flat_ids[:, None] == flat_ids[None, :]) & earlier
    rank = jnp.sum(same.astype(jnp.int32), axis=1)
    return (flat_ids * capacity + rank).reshape(expert_ids.shape)


def shards(
    gen_cache,
    prompt_cache,
    ancestors,
    queries,
    new_kv,
    tokens_in,
    norm_gain,
    routes,
    gate_weights,
    w_gate_up,
    w_down,
):
    ep_count = lax.axis_size(EP)
    per_dev = gen_cache.shape[0]
    row_count = 2 * per_dev
    width = tokens_in.shape[2]
    top_count = routes.shape[3]
    half_cols = w_down.shape[1]
    per_expert = 2
    slot_count = ep_count * per_expert

    in_own = w_gate_up.reshape(width, 2 * half_cols).T
    out_own = w_down.reshape(half_cols, width)
    own = jnp.concatenate([in_own, out_own], axis=0)
    before, after, low, high = ring_gather(own)

    piece_len = gen_cache.size // (per_dev * ep_count)
    flat_cache = (
        gen_cache.reshape(per_dev, ep_count, piece_len)
        .transpose(1, 0, 2)
        .reshape(ep_count, 2, per_dev * piece_len // 2)
    )
    flat_len = flat_cache.shape[2]
    fours = ancestors.reshape(2, per_dev // 2)
    digits = jnp.concatenate([fours // 256, fours % 256], axis=1).astype(jnp.bfloat16)
    side = jnp.pad(digits, ((0, 0), (0, 128 - digits.shape[1])))
    flat_cache = jnp.concatenate(
        [flat_cache, jnp.broadcast_to(side, (ep_count,) + side.shape)], axis=2
    )
    pieces = lax.all_to_all(flat_cache, EP, split_axis=0, concat_axis=0, tiled=True)
    chosen = resample(pieces, flat_len)
    moved = lax.all_to_all(chosen, EP, split_axis=0, concat_axis=0, tiled=True)
    cache_out = (
        moved.reshape(ep_count, per_dev, piece_len).transpose(1, 0, 2).reshape(gen_cache.shape)
    )
    attn_out = attend(queries, cache_out, new_kv, prompt_cache)

    values_f = tokens_in.astype(jnp.float32).reshape(row_count, width)
    normed = (
        values_f
        * lax.rsqrt(jnp.mean(values_f * values_f, axis=-1, keepdims=True) + 1e-06)
        * norm_gain
    ).astype(jnp.bfloat16)
    rep_place = lax.axis_index("rep")
    own_routes = lax.dynamic_index_in_dim(routes, rep_place, 0, keepdims=False).reshape(
        -1, top_count
    )
    own_gates = lax.dynamic_index_in_dim(gate_weights, rep_place, 0, keepdims=False).reshape(
        -1, top_count
    )
    labels = jnp.pad(own_routes.astype(jnp.bfloat16), ((0, 0), (0, 128 - top_count)))
    blocks = ring_rows(jnp.concatenate([normed, labels], axis=1))
    planes = lax.axis_size(PLANES)
    local = ep_count // planes
    packed = select_rows(lax.axis_index(PLANES), blocks, width, slot_count)
    rows = lax.all_to_all(
        packed.reshape(local, planes * per_expert, width),
        EP[2:],
        split_axis=0,
        concat_axis=0,
        tiled=True,
    ).reshape(slot_count, width)
    produced = expert(rows, own, before, after, low, high)

    slot_ids = slot_numbers(own_routes, per_expert)
    hits = jnp.arange(slot_count, dtype=jnp.int32)[:, None, None] == slot_ids[None, :, :]
    gate_of_slot = jnp.sum(jnp.where(hits, own_gates[None, :, :], 0.0), axis=-1).T
    came_back = lax.all_to_all(produced, EP, split_axis=0, concat_axis=0, tiled=True)
    came_back = came_back.reshape(slot_count, width)
    summed = jnp.dot(
        gate_of_slot,
        came_back.astype(jnp.float32),
        precision=lax.Precision.HIGHEST,
        preferred_element_type=jnp.float32,
    )
    expert_out = summed.astype(jnp.bfloat16).reshape(per_dev, 2, width)
    return (cache_out, attn_out, expert_out)


def solution(mesh):
    torus = Mesh(mesh.devices.reshape(mesh.shape["rep"], 4, 4, 4, 2), REP_EP)
    placed = (
        P(REP_EP, None, None, None, None),
        P(),
        P(REP_EP),
        P(REP_EP, None, None, None),
        P(REP_EP, None, None, None, None),
        P(REP_EP, None, None),
        P(),
        P(None, EP, None, None),
        P(None, EP, None, None),
        P(EP, None, None, "rep"),
        P(EP, "rep", None),
    )
    return jax.shard_map(
        shards,
        mesh=torus,
        in_specs=placed,
        out_specs=(
            P(REP_EP, None, None, None, None),
            P(REP_EP, None, None, None),
            P(REP_EP, None, None),
        ),
        check_vma=False,
    )
```

```python
import math

import jax
import jax.numpy as jnp
from jax import lax
from jax.experimental import pallas as pl
from jax.experimental.pallas import tpu as pltpu
from jax.sharding import Mesh
from jax.sharding import PartitionSpec as P


EP = ("ep_0", "ep_1", "ep_2")
REP_EP = ("rep",) + EP


def shift(block, axis, count, step):
    return lax.ppermute(block, axis, [(i, (i + step) % count) for i in range(count)])


def ring_gather(block):
    half = block.shape[0] // 2
    before = shift(block, "rep", 4, 1)
    after = shift(block, "rep", 4, -1)
    far_low = shift(before[:half], "rep", 4, 1)
    far_high = shift(after[half:], "rep", 4, -1)
    return before, after, far_low, far_high


def pack_body(tokens, gain, routes, cache, side, out_ref):
    width = tokens.shape[2]
    rows = tokens.shape[0] * tokens.shape[1]
    devices, two, _ = out_ref.shape
    slots = devices * two
    values = tokens[...].astype(jnp.float32).reshape(rows, width)
    scale = lax.rsqrt(jnp.mean(values * values, axis=-1, keepdims=True) + 1e-06)
    normed = (values * scale * gain[...]).astype(jnp.bfloat16)
    slot = lax.broadcasted_iota(jnp.int32, (rows, slots), 1)
    ids = routes[...]
    named = ids[:, 0:1] == slot // 2
    for k in range(1, ids.shape[1]):
        named = named | (ids[:, k : k + 1] == slot // 2)
    named = named.astype(jnp.float32)
    earlier = lax.broadcasted_iota(jnp.int32, (rows, rows), 1) < lax.broadcasted_iota(
        jnp.int32, (rows, rows), 0
    )
    rank = jnp.dot(earlier.astype(jnp.float32), named, preferred_element_type=jnp.float32)
    chosen = jnp.where(rank.astype(jnp.int32) == slot % 2, named, 0.0).astype(jnp.bfloat16)
    picked = lax.dot_general(
        chosen, normed, (((0,), (0,)), ((), ())), preferred_element_type=jnp.float32
    )
    out_ref[:, :, :width] = picked.astype(jnp.bfloat16).reshape(devices, two, width)
    half = cache.shape[0] // 2
    to = lax.broadcasted_iota(jnp.int32, (slots, devices), 0)
    come = lax.broadcasted_iota(jnp.int32, (slots, devices), 1)
    woven = None
    for k in range(two):
        wide = jnp.concatenate([cache[k * half + m] for m in range(half)], axis=1)
        place = (to == come * 2 + k).astype(jnp.float32).astype(jnp.bfloat16)
        part = jnp.dot(place, wide, preferred_element_type=jnp.float32)
        woven = part if woven is None else woven + part
    length = woven.shape[1]
    out_ref[:, :, width : width + length] = (
        woven.astype(jnp.bfloat16).reshape(devices, two, length)
    )
    out_ref[:, :, width + length :] = jnp.broadcast_to(
        side[...].reshape(1, two, side.shape[1]), (devices, two, side.shape[1])
    )


def pack(tokens, gain, routes, cache, side):
    width = tokens.shape[2]
    total = width + cache.shape[0] * cache.shape[2] // 2 + side.shape[1]
    spec = pl.BlockSpec(memory_space=pltpu.VMEM)
    return pl.pallas_call(
        pack_body,
        out_shape=jax.ShapeDtypeStruct((cache.shape[1], 2, total), jnp.bfloat16),
        in_specs=[spec] * 5,
        out_specs=spec,
        name="pack",
    )(tokens, gain.reshape(1, width), routes, cache, side)


def expert_body(
    rows_hbm, own_hbm, before_hbm, after_hbm, low_hbm, high_hbm, result,
    rows, own, before, after, far, sems,
):
    hidden = own.shape[0] // 3
    half = low_hbm.shape[0]
    copies = [
        pltpu.make_async_copy(src, dst, sems.at[n])
        for n, (src, dst) in enumerate(
            (
                (rows_hbm.at[:, :, : rows.shape[2]], rows),
                (own_hbm, own),
                (before_hbm, before),
                (after_hbm, after),
                (low_hbm, far.at[:half]),
                (high_hbm, far.at[half:]),
            )
        )
    ]
    for copy in copies:
        copy.start()
    total = None
    contract = (((1,), (1,)), ((), ()))
    for weights, waits in ((own, (0, 1)), (before, (2,)), (after, (3,)), (far, (4, 5))):
        for n in waits:
            copies[n].wait()
        if total is None:
            tokens = rows[...].reshape(rows.shape[0] * rows.shape[1], rows.shape[2])
        both = lax.dot_general(
            tokens, weights[: 2 * hidden], contract, preferred_element_type=jnp.float32
        )
        gate, upward = both[:, :hidden], both[:, hidden:]
        act = (gate / (1.0 + jnp.exp(-gate)) * upward).astype(jnp.bfloat16)
        part = jnp.dot(act, weights[2 * hidden :], preferred_element_type=jnp.float32)
        total = part if total is None else total + part
    result[...] = total.astype(jnp.bfloat16).reshape(result.shape)


def expert(rows, own, before, after, low, high):
    count, width = 2 * rows.shape[0], own.shape[1]
    return pl.pallas_call(
        expert_body,
        out_shape=jax.ShapeDtypeStruct((count // 2, 2, width), jnp.bfloat16),
        in_specs=[pl.BlockSpec(memory_space=pl.ANY)] + [pl.BlockSpec(memory_space=pltpu.HBM)] * 5,
        out_specs=pl.BlockSpec(memory_space=pltpu.VMEM),
        scratch_shapes=[pltpu.VMEM((count // 2, 2, width), jnp.bfloat16)]
        + [pltpu.VMEM(own.shape, jnp.bfloat16)] * 4
        + [pltpu.SemaphoreType.DMA((6,))],
        compiler_params=pltpu.CompilerParams(vmem_limit_bytes=32 * 1024 * 1024),
        name="expert",
    )(rows, own, before, after, low, high)


def resample_body(pieces_any, out_ref, pieces_ref, sem):
    first = pieces_any.shape[2] - pieces_ref.shape[2]
    copy = pltpu.make_async_copy(pieces_any.at[:, :, first:], pieces_ref, sem)
    copy.start()
    copy.wait()
    devices, two, width = pieces_ref.shape
    count, length = devices * two, out_ref.shape[2]
    rows = pieces_ref[...].reshape(count, width)
    digits = rows[:, length : length + 8].astype(jnp.float32).astype(jnp.int32)
    parents = digits[:, :4] * 256 + digits[:, 4:]
    piece = length // 4
    stacked = jnp.concatenate([rows[:, m * piece : (m + 1) * piece] for m in range(4)], axis=0)
    column = lax.broadcasted_iota(jnp.int32, (count, 4 * count), 1)
    particle = column % count * 4 + column // count
    chosen = []
    for m in range(4):
        onehot = (parents[:, m : m + 1] == particle).astype(jnp.float32).astype(jnp.bfloat16)
        picked = jnp.dot(onehot, stacked, preferred_element_type=jnp.float32)
        chosen.append(picked.astype(jnp.bfloat16))
    out_ref[...] = jnp.concatenate(chosen, axis=1).reshape(out_ref.shape)


def resample(pieces, length):
    return pl.pallas_call(
        resample_body,
        out_shape=jax.ShapeDtypeStruct(pieces.shape[:2] + (length,), jnp.bfloat16),
        in_specs=[pl.BlockSpec(memory_space=pl.ANY)],
        out_specs=pl.BlockSpec(memory_space=pltpu.VMEM),
        scratch_shapes=[
            pltpu.VMEM(pieces.shape[:2] + (length + 128,), jnp.bfloat16),
            pltpu.SemaphoreType.DMA(()),
        ],
        name="resample",
    )(pieces)


def attend(queries, gen_block, new_block, prompt_cache):
    count = queries.shape[0]
    heads = queries.shape[2]
    head_dim = queries.shape[3]
    kv_heads = new_block.shape[3]
    score_scale = 1.0 / math.sqrt(head_dim)
    grouped = queries.reshape(count, 2, kv_heads, heads // kv_heads, head_dim)
    prompt_scores = (
        jnp.einsum(
            "btngd,snd->btngs", grouped, prompt_cache[:, 0], preferred_element_type=jnp.float32
        )
        * score_scale
    )
    gen_scores = (
        jnp.einsum(
            "btngd,bsnd->btngs", grouped, gen_block[:, :, 0], preferred_element_type=jnp.float32
        )
        * score_scale
    )
    new_scores = (
        jnp.einsum(
            "btngd,bsnd->btngs", grouped, new_block[:, :, 0], preferred_element_type=jnp.float32
        )
        * score_scale
    )
    causal = lax.broadcasted_iota(jnp.int32, (2, 2), 1) <= lax.broadcasted_iota(
        jnp.int32, (2, 2), 0
    )
    new_scores = jnp.where(causal[None, :, None, None, :], new_scores, -jnp.inf)
    row_max = jnp.maximum(
        jnp.maximum(prompt_scores.max(-1), gen_scores.max(-1)), new_scores.max(-1)
    )[..., None]
    prompt_exp = jnp.exp(prompt_scores - row_max)
    gen_exp = jnp.exp(gen_scores - row_max)
    new_exp = jnp.exp(new_scores - row_max)
    denom = (prompt_exp.sum(-1) + gen_exp.sum(-1) + new_exp.sum(-1))[..., None]
    prompt_weights = (prompt_exp / denom).astype(jnp.bfloat16)
    gen_weights = (gen_exp / denom).astype(jnp.bfloat16)
    new_weights = (new_exp / denom).astype(jnp.bfloat16)
    result = jnp.einsum(
        "btngs,snd->btngd", prompt_weights, prompt_cache[:, 1], preferred_element_type=jnp.float32
    )
    result = result + jnp.einsum(
        "btngs,bsnd->btngd", gen_weights, gen_block[:, :, 1], preferred_element_type=jnp.float32
    )
    result = result + jnp.einsum(
        "btngs,bsnd->btngd", new_weights, new_block[:, :, 1], preferred_element_type=jnp.float32
    )
    return result.reshape(count, 2, heads, head_dim).astype(jnp.bfloat16)


def slot_numbers(expert_ids, capacity):
    flat_ids = expert_ids.reshape(-1)
    count = flat_ids.shape[0]
    earlier = lax.broadcasted_iota(jnp.int32, (count, count), 1) < lax.broadcasted_iota(
        jnp.int32, (count, count), 0
    )
    same = (flat_ids[:, None] == flat_ids[None, :]) & earlier
    rank = jnp.sum(same.astype(jnp.int32), axis=1)
    return (flat_ids * capacity + rank).reshape(expert_ids.shape)


def shards(
    gen_cache,
    prompt_cache,
    ancestors,
    queries,
    new_kv,
    tokens_in,
    norm_gain,
    routes,
    gate_weights,
    w_gate_up,
    w_down,
):
    ep_count = lax.axis_size(EP)
    per_dev = gen_cache.shape[0]
    width = tokens_in.shape[2]
    top_count = routes.shape[3]
    half_cols = w_down.shape[1]
    per_expert = 2
    slot_count = ep_count * per_expert

    in_own = w_gate_up.reshape(width, 2 * half_cols).T
    out_own = w_down.reshape(half_cols, width)
    own = jnp.concatenate([in_own, out_own], axis=0)
    before, after, low, high = ring_gather(own)

    rep_place = lax.axis_index("rep")
    own_routes = lax.dynamic_index_in_dim(routes, rep_place, 0, keepdims=False).reshape(
        -1, top_count
    )
    own_gates = lax.dynamic_index_in_dim(gate_weights, rep_place, 0, keepdims=False).reshape(
        -1, top_count
    )
    piece_len = gen_cache.size // (per_dev * ep_count)
    flat_len = per_dev * piece_len // 2
    fours = ancestors.reshape(2, per_dev // 2)
    digits = jnp.concatenate([fours // 256, fours % 256], axis=1).astype(jnp.bfloat16)
    side = jnp.pad(digits, ((0, 0), (0, 128 - digits.shape[1])))
    outgoing = pack(
        tokens_in, norm_gain, own_routes, gen_cache.reshape(per_dev, ep_count, piece_len), side
    )
    received = lax.all_to_all(outgoing, EP, split_axis=0, concat_axis=0, tiled=True)
    chosen = resample(received, flat_len)
    moved = lax.all_to_all(chosen, EP, split_axis=0, concat_axis=0, tiled=True)
    cache_out = (
        moved.reshape(ep_count, per_dev, piece_len).transpose(1, 0, 2).reshape(gen_cache.shape)
    )
    attn_out = attend(queries, cache_out, new_kv, prompt_cache)

    produced = expert(received, own, before, after, low, high)

    slot_ids = slot_numbers(own_routes, per_expert)
    hits = jnp.arange(slot_count, dtype=jnp.int32)[:, None, None] == slot_ids[None, :, :]
    gate_of_slot = jnp.sum(jnp.where(hits, own_gates[None, :, :], 0.0), axis=-1).T
    came_back = lax.all_to_all(produced, EP, split_axis=0, concat_axis=0, tiled=True)
    came_back = came_back.reshape(slot_count, width)
    summed = jnp.dot(
        gate_of_slot,
        came_back.astype(jnp.float32),
        precision=lax.Precision.HIGHEST,
        preferred_element_type=jnp.float32,
    )
    expert_out = summed.astype(jnp.bfloat16).reshape(per_dev, 2, width)
    return (cache_out, attn_out, expert_out)


def solution(mesh):
    torus = Mesh(mesh.devices.reshape(mesh.shape["rep"], 16, 4, 2), REP_EP)
    placed = (
        P(REP_EP, None, None, None, None),
        P(),
        P(REP_EP),
        P(REP_EP, None, None, None),
        P(REP_EP, None, None, None, None),
        P(REP_EP, None, None),
        P(),
        P(None, EP, None, None),
        P(None, EP, None, None),
        P(EP, None, None, "rep"),
        P(EP, "rep", None),
    )
    return jax.shard_map(
        shards,
        mesh=torus,
        in_specs=placed,
        out_specs=(
            P(REP_EP, None, None, None, None),
            P(REP_EP, None, None, None),
            P(REP_EP, None, None),
        ),
        check_vma=False,
    )
```
